32 devices in a mesh: grid: 16 (over z, x, core), band: 2 (over y).
Axes of the slice: x: 2, y: 2, z: 4, core: 2. Of those that a mesh axis runs over, the one named last changes fastest.
Arguments:
- left_bands: float32 [2, 8, 128, 128, 128], P(None, 'band', 'grid'), may hold values from -6 to 6
- right_bands: float32 [2, 4, 128, 128, 128], P(None, 'band', 'grid'), may hold values from -6 to 6
- sphere_index: int32 [16384], replicated, may hold values from 0 to 2097151, as said below
- right_order: int32 [4], replicated, may hold values from 0 to 3, each once
Outputs:
- pair_density: float32 [2, 8, 4, 16384], P(None, 'band', None, 'grid')
The draws below stay inside these ranges and needn't reach their ends.
Inputs may be any that keep to these rules, and one draw needn't show every extreme that they name: `sphere_index`: flat index (kz * 128 + ky) * 128 + kx; an index may repeat. In each aligned block of 1024 entries, at most 64 entries share one value of ky // 8, and some value is shared by exactly 64. `right_order`: each second band once.
All inputs are finite; a program needn't handle non-finite values.
Results may differ from the reference program's by a relative error of at most 0.00008.
Values sent between devices are 32-bit elements; how exact they have to be, the bound alone decides.
A program may use at most 256 MiB of HBM per device.

```python
import jax
import jax.numpy as jnp
from jax import lax

NG = 128
NX = 128
NGV = 16384
NL = 8
NR = 4
ZS = 8


def draw_sphere_index(key, part):
    devices = NG // ZS
    per_block = NGV // devices
    key_shift = jax.random.fold_in(key, 11)
    key_perm = jax.random.fold_in(key, 12)
    key_row = jax.random.fold_in(key, 13)
    key_plane = jax.random.fold_in(key, 14)
    key_column = jax.random.fold_in(key, 15)
    shifts = jax.random.randint(key_shift, (devices, 1), 0, devices)
    position = jnp.arange(per_block, dtype=jnp.int32)[None, :]
    source = (position + shifts) % devices
    block_keys = jax.random.split(key_perm, devices)
    orders = jax.vmap(lambda k: jax.random.permutation(k, per_block))(block_keys)
    source = jnp.take_along_axis(source, orders.astype(jnp.int32), axis=1).reshape(-1)
    wave_y = source * ZS + jax.random.randint(key_row, (NGV,), 0, ZS)
    wave_z = jax.random.randint(key_plane, (NGV,), 0, NG)
    wave_x = jax.random.randint(key_column, (NGV,), 0, NX)
    return ((wave_z * NG + wave_y) * NX + wave_x).astype(jnp.int32)


def levels(stream_key, shape, shards, low, top_value):
    def one(dim, parts):
        draws = jax.random.uniform(jax.random.fold_in(jax.random.fold_in(stream_key, 6), dim), (parts,), jnp.float32, low / len(shards), top_value / len(shards))
        return jnp.repeat(jnp.exp(draws), shape[dim] // parts).reshape((-1,) + (1,) * (len(shape) - dim - 1))

    factor_of = one(*shards[0])
    for cut in shards[1:]:
        factor_of = factor_of * one(*cut)
    return factor_of


def normal_values(stream_key, dims, scale, reach, cuts=(), kind=jnp.bfloat16):
    array = jax.random.normal(stream_key, dims, jnp.float32) * scale
    if len(cuts) > 0:
        array = levels(stream_key, dims, cuts, -0.22, 0.18) * array
    return jnp.clip(array, min=-reach, max=reach).astype(kind)


def setup_inputs(seed: int = 0) -> dict:
    key_list = jax.random.split(jax.random.key(seed), 5)
    return {
        "left_bands": normal_values(key_list[0], (2, NL, NG, NG, NX), 1.0, 6.0, ((1, 2), (2, 16)), jnp.float32),
        "right_bands": normal_values(key_list[1], (2, NR, NG, NG, NX), 1.0, 6.0, ((1, 2), (2, 16)), jnp.float32),
        "sphere_index": draw_sphere_index(jax.random.fold_in(key_list[4], 71), 0),
        "right_order": jax.random.permutation(key_list[3], NR).astype(jnp.int32),
    }


def reference(left_bands, right_bands, sphere_index, right_order):
    factor = 1.0 / (NG * NG * NX) ** 0.5

    def one_left(left_field):
        def one_right(column):
            right_field = lax.dynamic_index_in_dim(right_bands, column, 1, keepdims=False)
            real_part = left_field[0] * right_field[0] + left_field[1] * right_field[1]
            imag_part = left_field[0] * right_field[1] - left_field[1] * right_field[0]
            spectrum = jnp.fft.fftn(real_part + 1j * imag_part)
            picked = spectrum.reshape(-1)[sphere_index]
            return jnp.stack([jnp.real(picked), jnp.imag(picked)]).astype(jnp.float32) * factor

        return lax.map(one_right, right_order)

    result = lax.map(one_left, jnp.moveaxis(left_bands, 1, 0))
    return jnp.transpose(result, (2, 0, 1, 3))
```

```python
import math

import jax
import jax.numpy as jnp
from jax import lax
from jax.sharding import PartitionSpec as P

HIGH = lax.Precision.HIGH
HIGHEST = lax.Precision.HIGHEST
F32 = jnp.float32
BF16 = jnp.bfloat16


def swapped(block, axis):
    count = lax.axis_size(axis)
    return lax.ppermute(block, axis, [(k, k ^ 1) for k in range(count)])


def dft_tables(length):
    counter = jnp.arange(length, dtype=jnp.int32)
    angles = (counter[:, None] * counter[None, :] % length).astype(F32) * (2.0 * math.pi / length)
    return (jnp.cos(angles), jnp.sin(angles))


def complex_matrix(length):
    cosine, sine = dft_tables(length)
    return jnp.concatenate(
        [jnp.concatenate([cosine, -sine], 1), jnp.concatenate([sine, cosine], 1)], 0
    ).reshape(2, length, 2, length)


def split(value):
    high = lax.reduce_precision(value, 8, 7)
    return high.astype(BF16), (value - high).astype(BF16)


def plan(sphere_index, grid, nx, n_dev):
    rows = grid // n_dev
    per = sphere_index.shape[0] // n_dev
    slots = max(1, per // n_dev)
    wave_z = sphere_index // (grid * nx)
    wave_y = sphere_index // nx % grid
    wave_x = sphere_index % nx
    source = (wave_y // rows).reshape(n_dev, per)
    onehot = (source[:, :, None] == jnp.arange(n_dev, dtype=jnp.int32)).astype(BF16)
    before = jnp.tril(jnp.ones((per, per), BF16), -1)
    counts = jnp.einsum("ij,bjs->bis", before, onehot, preferred_element_type=F32)
    rank = jnp.sum(counts * onehot, axis=2).astype(jnp.int32)
    slot = source * slots + rank
    column = (wave_y % rows) * nx + wave_x
    packed = (wave_z * (rows * nx) + column).reshape(n_dev, per)
    target = jnp.arange(n_dev * slots, dtype=jnp.int32)
    chosen = jnp.sum(
        jnp.where(slot[:, :, None] == target[None, None, :], packed[:, :, None] + 1, 0), axis=1
    ) - 1
    chosen = chosen.reshape(n_dev, n_dev, slots).transpose(1, 0, 2).reshape(n_dev, n_dev * slots)
    return chosen, slot


def local(left_bands, right_bands, sphere_index, right_order):
    n_dev = lax.axis_size("grid")
    me = lax.axis_index("grid")
    nl, zs, ng, nx = left_bands.shape[1:]
    own_right = right_bands.shape[1]
    rows = ng // n_dev
    per = sphere_index.shape[0] // n_dev
    slots = max(1, per // n_dev)
    chosen, slot = plan(sphere_index, ng, nx, n_dev)
    points = n_dev * slots
    filled = chosen >= 0
    col = jnp.where(filled, chosen % (rows * nx), -1)
    kz = chosen // (rows * nx)
    hot = (jnp.arange(rows * nx, dtype=jnp.int32)[None, :, None] == col[:, None, :]).astype(BF16)
    plane = me * zs + jnp.arange(zs, dtype=jnp.int32)
    angle = (plane[None, :, None] * kz[:, None, :] % ng).astype(F32) * (2.0 * math.pi / ng)
    scale = 1.0 / (ng * ng * nx) ** 0.5
    cos_z, sin_z = jnp.cos(angle) * scale, jnp.sin(angle) * scale
    wx, wy = complex_matrix(nx), complex_matrix(ng)

    def partial(right):
        nr = right.shape[1]
        l0, l1 = left_bands[0][:, None], left_bands[1][:, None]
        r0, r1 = right[0][None], right[1][None]
        pair = jnp.stack([l0 * r0 + l1 * r1, l0 * r1 - l1 * r0])
        pair = pair.reshape(2, nl * nr, zs, ng, nx)
        pair = jnp.einsum("cpzyx,cxdk->dpzyk", pair, wx, precision=HIGH)
        pair = jnp.einsum("cpzyk,cydq->dpzqk", pair, wy, precision=HIGH)
        high, low = split(pair.reshape(2, nl * nr, zs, n_dev, rows * nx))
        form = "dpzsc,scq->sdpzq"
        got = jnp.einsum(form, high, hot, preferred_element_type=F32) + jnp.einsum(
            form, low, hot, preferred_element_type=F32
        )
        c, s = cos_z[:, None], sin_z[:, None]
        out_r = jnp.sum(got[:, 0] * c + got[:, 1] * s, axis=2)
        out_i = jnp.sum(got[:, 1] * c - got[:, 0] * s, axis=2)
        out = jnp.stack([out_r, out_i], 0)
        out = out.reshape(2, n_dev, nl * nr, n_dev, slots).transpose(3, 0, 2, 1, 4)
        out = out.reshape(n_dev, 2 * nl * nr, n_dev * slots)
        got = lax.psum_scatter(out, "grid", scatter_dimension=0, tiled=False)
        return got.reshape(2, nl, nr, n_dev * slots)

    other = swapped(right_bands, "band")
    mine = partial(right_bands)
    theirs = partial(other)
    result = jnp.concatenate([mine, theirs], axis=2)
    own_slot = lax.dynamic_index_in_dim(slot, me, 0, keepdims=False)
    pick = (jnp.arange(n_dev * slots, dtype=jnp.int32)[:, None] == own_slot[None, :]).astype(F32)
    result = jnp.einsum("dnmt,ti->dnmi", result, pick, precision=HIGHEST)
    position = (right_order - lax.axis_index("band") * own_right) % right_order.shape[0]
    return jnp.take(result, position, axis=2)


def solution(mesh):
    placed = (P(None, "band", "grid", None, None), P(None, "band", "grid", None, None), P(), P())
    return jax.shard_map(
        local, mesh=mesh, in_specs=placed, out_specs=P(None, "band", None, "grid"), check_vma=False
    )
```

```python
import math

import jax
import jax.numpy as jnp
from jax import lax
from jax.experimental import pallas as pl
from jax.experimental.pallas import tpu as pltpu
from jax.sharding import PartitionSpec as P

HIGH = lax.Precision.HIGH
HIGHEST = lax.Precision.HIGHEST
F32 = jnp.float32
BF16 = jnp.bfloat16


def swapped(block, axis):
    count = lax.axis_size(axis)
    return lax.ppermute(block, axis, [(k, k ^ 1) for k in range(count)])


def dft_tables(length):
    counter = jnp.arange(length, dtype=jnp.int32)
    angles = (counter[:, None] * counter[None, :] % length).astype(F32) * (2.0 * math.pi / length)
    return (jnp.cos(angles), jnp.sin(angles))


def complex_matrix(length):
    cosine, sine = dft_tables(length)
    return jnp.concatenate(
        [jnp.concatenate([cosine, -sine], 1), jnp.concatenate([sine, cosine], 1)], 0
    ).reshape(2, length, 2, length)


def split(value):
    high = lax.reduce_precision(value, 8, 7)
    return high.astype(BF16), (value - high).astype(BF16)


def plan(sphere_index, grid, nx, n_dev):
    rows = grid // n_dev
    per = sphere_index.shape[0] // n_dev
    slots = max(1, per // n_dev)
    wave_z = sphere_index // (grid * nx)
    wave_y = sphere_index // nx % grid
    wave_x = sphere_index % nx
    source = (wave_y // rows).reshape(n_dev, per)
    onehot = (source[:, :, None] == jnp.arange(n_dev, dtype=jnp.int32)).astype(BF16)
    before = jnp.tril(jnp.ones((per, per), BF16), -1)
    counts = jnp.einsum("ij,bjs->bis", before, onehot, preferred_element_type=F32)
    rank = jnp.sum(counts * onehot, axis=2).astype(jnp.int32)
    slot = source * slots + rank
    column = (wave_y % rows) * nx + wave_x
    packed = (wave_z * (rows * nx) + column).reshape(n_dev, per)
    target = jnp.arange(n_dev * slots, dtype=jnp.int32)
    chosen = jnp.sum(
        jnp.where(slot[:, :, None] == target[None, None, :], packed[:, :, None] + 1, 0), axis=1
    ) - 1
    bits = n_dev.bit_length() - 1
    if n_dev == 1 << bits:
        chosen = chosen.reshape((2,) * bits + (n_dev * slots,))
        chosen = chosen.transpose(tuple(range(bits))[::-1] + (bits,))
    chosen = chosen.reshape(n_dev, n_dev, slots).transpose(1, 0, 2).reshape(n_dev, n_dev * slots)
    return chosen, slot


def select_body(field_ref, col_ref, cos_ref, sin_ref, out_ref, parts_ref):
    count, rows, nx = field_ref.shape
    planes = cos_ref.shape[1]
    points = col_ref.shape[2]
    flat = field_ref.reshape(count * rows, nx)
    for row in range(rows):
        value = flat[pl.ds(row, count, stride=rows), :]
        high = value.astype(BF16)
        low = (value - high.astype(F32)).astype(BF16)
        parts_ref[0:count, row * nx : (row + 1) * nx] = high
        parts_ref[count : 2 * count, row * nx : (row + 1) * nx] = low
    tile = min(points, 256)

    def step(index, carry):
        span = pl.ds(pl.multiple_of(index * tile, tile), tile)
        col = col_ref[0, :, span]
        place = lax.broadcasted_iota(jnp.int32, (rows * nx, tile), 0)
        hot = jnp.where(place == col, 1.0, 0.0).astype(BF16)
        both = jnp.dot(parts_ref[...], hot, preferred_element_type=F32)
        got = (both[:count] + both[count:]).reshape(2, count // (2 * planes), planes, tile)
        cosine, sine = cos_ref[0, :, span][None], sin_ref[0, :, span][None]
        real = jnp.sum(got[0] * cosine + got[1] * sine, axis=1)
        imag = jnp.sum(got[1] * cosine - got[0] * sine, axis=1)
        out_ref[0, :, span] = jnp.concatenate([real, imag], axis=0)
        return carry

    lax.fori_loop(0, points // tile, step, 0)


def select_sum(field, col, cos_z, sin_z):
    two, pairs, planes, ng, nx = field.shape
    groups, points = col.shape
    rows = ng // groups
    if rows % 8 == 0 and planes % 8 == 0 and nx % 128 == 0 and points % 256 == 0:
        count = two * pairs * planes
        flops = 4 * count * rows * nx * points * groups
        return pl.pallas_call(
            select_body,
            grid=(groups,),
            in_specs=[
                pl.BlockSpec((count, rows, nx), lambda g: (0, g, 0)),
                pl.BlockSpec((1, 1, points), lambda g: (g, 0, 0)),
                pl.BlockSpec((1, planes, points), lambda g: (g, 0, 0)),
                pl.BlockSpec((1, planes, points), lambda g: (g, 0, 0)),
            ],
            out_specs=pl.BlockSpec((1, 2 * pairs, points), lambda g: (g, 0, 0)),
            out_shape=jax.ShapeDtypeStruct((groups, 2 * pairs, points), F32),
            scratch_shapes=[pltpu.VMEM((2 * count, rows * nx), BF16)],
            cost_estimate=pl.CostEstimate(
                flops=flops, bytes_accessed=4 * count * ng * nx, transcendentals=0
            ),
        )(field.reshape(count, ng, nx), col[:, None, :], cos_z, sin_z)
    high, low = split(field.reshape(2, pairs, planes, groups, rows * nx))
    place = jnp.arange(rows * nx, dtype=jnp.int32)[None, :, None]
    hot = (place == col[:, None, :]).astype(BF16)
    form = "dpzsc,scq->sdpzq"
    got = jnp.einsum(form, high, hot, preferred_element_type=F32) + jnp.einsum(
        form, low, hot, preferred_element_type=F32
    )
    c, s = cos_z[:, None], sin_z[:, None]
    real = jnp.sum(got[:, 0] * c + got[:, 1] * s, axis=2)
    imag = jnp.sum(got[:, 1] * c - got[:, 0] * s, axis=2)
    return jnp.concatenate([real, imag], axis=1)


def summed_over_grid(part, me, n_dev):
    groups, values, points = part.shape
    bits = n_dev.bit_length() - 1
    if n_dev == 1 << bits:
        for bit in range(bits):
            half = part.shape[2] // 2
            lower, upper = part[:, :, :half], part[:, :, half:]
            mine = me // (1 << bit) % 2 == 1
            route = [(k, k ^ (1 << bit)) for k in range(n_dev)]
            arrived = lax.ppermute(jnp.where(mine, lower, upper), "grid", route)
            part = jnp.where(mine, upper, lower) + arrived
        return part
    part = part.reshape(groups, values, n_dev, points // n_dev).transpose(2, 0, 1, 3)
    return lax.psum_scatter(part, "grid", scatter_dimension=0, tiled=False)


def local(left_bands, right_bands, sphere_index, right_order):
    n_dev = lax.axis_size("grid")
    me = lax.axis_index("grid")
    nl, zs, ng, nx = left_bands.shape[1:]
    own_right = right_bands.shape[1]
    rows = ng // n_dev
    other = swapped(right_bands, "band")
    chosen, slot = plan(sphere_index, ng, nx, n_dev)
    filled = chosen >= 0
    col = jnp.where(filled, chosen % (rows * nx), -1)
    kz = chosen // (rows * nx)
    plane = me * zs + jnp.arange(zs, dtype=jnp.int32)
    angle = (plane[None, :, None] * kz[:, None, :] % ng).astype(F32) * (2.0 * math.pi / ng)
    scale = 1.0 / (ng * ng * nx) ** 0.5
    cos_z, sin_z = jnp.cos(angle) * scale, jnp.sin(angle) * scale
    wx, wy = complex_matrix(nx), complex_matrix(ng)

    def partial(right):
        nr = right.shape[1]
        l0, l1 = left_bands[0][:, None], left_bands[1][:, None]
        r0, r1 = right[0][None], right[1][None]
        pair = jnp.stack([l0 * r0 + l1 * r1, l0 * r1 - l1 * r0])
        pair = pair.reshape(2, nl * nr, zs, ng, nx)
        pair = jnp.einsum("cpzyx,cxdk->dpzyk", pair, wx, precision=HIGH)
        pair = jnp.einsum("cpzyk,cydq->dpzqk", pair, wy, precision=HIGH)
        return select_sum(pair, col, cos_z, sin_z)

    first = partial(right_bands)
    first, other = lax.optimization_barrier((first, other))
    second = partial(other)
    halves = []
    for part in (first, second):
        got = summed_over_grid(part, me, n_dev)
        got = got.transpose(1, 0, 2).reshape(2, nl, own_right, -1)
        halves.append(got)
    result = jnp.concatenate(halves, axis=2)
    own_slot = lax.dynamic_index_in_dim(slot, me, 0, keepdims=False)
    place = jnp.arange(result.shape[3], dtype=jnp.int32)
    pick = (place[:, None] == own_slot[None, :]).astype(F32)
    result = jnp.einsum("dnmt,ti->dnmi", result, pick, precision=HIGHEST)
    position = (right_order - lax.axis_index("band") * own_right) % right_order.shape[0]
    return jnp.take(result, position, axis=2)


def solution(mesh):
    placed = (P(None, "band", "grid", None, None), P(None, "band", "grid", None, None), P(), P())
    return jax.shard_map(
        local, mesh=mesh, in_specs=placed, out_specs=P(None, "band", None, "grid"), check_vma=False
    )
```
